32 devices in a mesh: gx: 8 (over z, y), gy: 4 (over x, core).
Axes of the slice: x: 2, y: 2, z: 4, core: 2. Of those that a mesh axis runs over, the one named last changes fastest.
Arguments:
- image_feats: bfloat16 [16384, 4096], P('gx', 'gy'), may hold values from -6 to 6
- w_kv: bfloat16 [4096, 2048], P('gy'), may hold values from -0.09375 to 0.09375
- k_gain: float32 [128], replicated, may hold values from 0.25 to 1.75
- tile_rows: int32 [128], replicated, may hold values from 0 to 128
- deal: int32 [8, 16], replicated, may hold values from 0 to 127, as said below
Outputs:
- keys_out: bfloat16 [16384, 1024], P('gx', 'gy')
- values_out: bfloat16 [16384, 1024], P('gx', 'gy')
The draws below stay inside these ranges and needn't reach their ends.
Inputs may be any that keep to these rules, and one draw needn't show every extreme that they name: Each input tile is named exactly once; deal[j, s] % 16 == s; two entries of one row j that name tiles of the same index of gx stand in columns s that differ by a multiple of 8, so one row names at most 2 tiles of one index of gx, and exactly 2 for some.
All inputs are finite; a program needn't handle non-finite values.
Results may differ from the reference program's by a relative error of at most 0.001.
Values may be sent and summed in bfloat16 or wider, within the bound.
No kernel may reach another device: no remote copies, remote signals or barrier semaphores. Data moves between devices by JAX's collectives and lax.ppermute only.
A program may use at most 128 MiB of HBM per device.

```python
import jax
import jax.numpy as jnp
from jax import lax

D = 4096
HEADS = 8
HD = 128
TILE = 128
TPD = 16
KV = 1024
TILES = 128
ROWS = 16384
N_GX = 8


def draw_deal(key, part):
    inner = jax.random.fold_in(key, 7)
    first_key, second_key = jax.random.split(inner)
    base = jax.random.permutation(first_key, N_GX)
    shuffled = jax.random.permutation(second_key, N_GX)
    slot_index = jnp.arange(TPD, dtype=jnp.int32)
    offsets = shuffled[slot_index % N_GX]
    column = jnp.arange(N_GX, dtype=jnp.int32)[:, None]
    source_device = base[(column + offsets[None, :]) % N_GX]
    return (source_device * TPD + slot_index[None, :]).astype(jnp.int32)


def with_ends(drawn, own_key, least, top_value):
    dims = drawn.shape
    spot = [jax.random.randint(jax.random.fold_in(own_key, axis), (), 0, dims[axis]) for axis in range(len(dims))]
    drawn = drawn.at[tuple(spot)].set(least)
    longest = dims.index(max(dims))
    spot[longest] = (spot[longest] + 1) % dims[longest]
    return drawn.at[tuple(spot)].set(top_value)


def shard_levels(own_key, shape, cuts, smallest, top_value):
    loudness, own = 1.0, jax.random.fold_in(own_key, 6)
    for dim, blocks in cuts:
        steps = jnp.exp(jax.random.uniform(jax.random.fold_in(own, dim), (blocks,), jnp.float32, smallest / len(cuts), top_value / len(cuts)))
        loudness = loudness * jnp.repeat(steps, shape[dim] // blocks).reshape([-1 if axis == dim else 1 for axis in range(len(shape))])
    return loudness


def scatter_about(stream_key, dims, deviation, reach, shards=(), kind=jnp.bfloat16):
    gain = shard_levels(stream_key, dims, shards, -0.22, 0.18) if shards else 1.0
    result = jax.random.normal(stream_key, dims, jnp.float32) * deviation * gain
    return jnp.minimum(jnp.maximum(result, -reach), reach).astype(kind)


def setup_inputs(seed: int = 0) -> dict:
    keys = jax.random.split(jax.random.key(seed), 6)
    image_feats = scatter_about(keys[0], (ROWS, D), 1.0, 6.0, ((0, 8), (1, 4)))
    w_kv = scatter_about(keys[1], (D, 2 * KV), D ** -0.5, 0.09375, ((0, 4),))
    k_gain = jnp.clip(1.0 + 0.15 * jax.random.normal(keys[2], (HD,), jnp.float32), 0.25, 1.75)
    tile_rows = with_ends(jax.random.randint(keys[3], (TILES,), 0, TILE + 1), jax.random.fold_in(keys[3], 1), 0, TILE).astype(jnp.int32)
    deal = draw_deal(jax.random.fold_in(keys[5], 71), 0)
    return {"image_feats": image_feats, "w_kv": w_kv, "k_gain": k_gain, "tile_rows": tile_rows, "deal": deal}


epsilon = 1e-05

def reference(image_feats, w_kv, k_gain, tile_rows, deal):
    tiled = image_feats.reshape(TILES, TILE, D)
    order = deal.reshape(-1).astype(jnp.int32)
    dealt = jnp.take(tiled, order, axis=0).reshape(ROWS, D)
    projected = jnp.dot(dealt, w_kv, preferred_element_type=jnp.float32)
    projected = projected.reshape(ROWS, 2, HEADS, HD)
    key_pre = projected[:, 0]
    value_pre = projected[:, 1]
    mean_square = lax.optimization_barrier(jnp.mean(key_pre * key_pre, axis=-1, keepdims=True))
    normed = key_pre * lax.rsqrt(mean_square + epsilon) * k_gain
    limits = jnp.take(tile_rows, order, axis=0)
    position = jnp.arange(TILE, dtype=jnp.int32)
    valid = (position[None, :] < limits[:, None]).reshape(ROWS, 1, 1)
    keys_out = jnp.where(valid, normed, 0.0).reshape(ROWS, KV).astype(jnp.bfloat16)
    values_out = jnp.where(valid, value_pre, 0.0).reshape(ROWS, KV).astype(jnp.bfloat16)
    return (keys_out, values_out)
```

```python
import functools

import jax
import jax.numpy as jnp
from jax import lax
from jax.experimental import pallas as pl
from jax.experimental.pallas import tpu as pltpu
from jax.sharding import PartitionSpec as P


HD = 128
TILE = 128
TPD = 16
CORES = 2
epsilon = 1e-05

STEPS = 64.0
TOP = 32700.0
PAD = 16

VMEM = pl.BlockSpec(memory_space=pltpu.VMEM)
SMEM = pl.BlockSpec(memory_space=pltpu.SMEM)
ANY = pl.BlockSpec(memory_space=pl.ANY)


def call(body, ins, outs, shapes, flops, scratch=()):
    nbytes = sum(s.size * s.dtype.itemsize for s in shapes)
    return pl.pallas_call(
        body,
        in_specs=ins,
        out_specs=outs,
        out_shape=shapes,
        scratch_shapes=scratch,
        cost_estimate=pl.CostEstimate(flops=int(flops), bytes_accessed=2 * nbytes, transcendentals=0),
    )


STAGES = ((3, "a2a"), (3, "permute"), (2, "a2a"))


def target(k):
    chips = lax.axis_size("gy") // CORES
    member = lax.axis_index("gy")
    chip, core = member // CORES, member % CORES
    there = (chip + k) % chips * CORES
    return there + core, there + 1 - core


def run_all(copies):
    for c in copies:
        c.start()
    for c in copies:
        c.wait()


def prepare_body(f_ref, w_ref, *refs, stages, ks, share):
    feats, weights, sem = refs[: len(stages)], refs[len(stages) : -1], refs[-1]
    members = lax.axis_size("gy")
    copies = []
    for i, k in enumerate(ks):
        for j, which in enumerate(target(k)):
            w_out = weights[2 * i + j]
            for part in range(2):
                start = pl.multiple_of((part * members + which) * share, share)
                copies.append((w_ref.at[:, pl.ds(start, share)], w_out.at[:, part * share : (part + 1) * share]))
    for (r, m), f_out in zip(stages, feats):
        copies.append((f_ref.at[:, r : r + m], f_out))
    run_all([pltpu.make_async_copy(a, b, sem.at[i]) for i, (a, b) in enumerate(copies)])


def prepare(feats, w_kv, stages, ks, share):
    width = feats.shape[2]
    shapes = [jax.ShapeDtypeStruct((TPD, m, width), feats.dtype) for _, m in stages]
    shapes += [jax.ShapeDtypeStruct((width, 2 * share), w_kv.dtype) for _ in range(2 * len(ks))]
    body = functools.partial(prepare_body, stages=stages, ks=ks, share=share)
    sems = [pltpu.SemaphoreType.DMA((len(stages) + 4 * len(ks),))]
    got = call(body, [ANY, ANY], [VMEM] * len(shapes), shapes, 1e6, sems)(feats, w_kv)
    weights = got[len(stages) :]
    return got[: len(stages)], weights[::2], weights[1::2]


def encode(total, out_ref, share):
    rows = total.shape[0]
    lane = lax.broadcasted_iota(jnp.int32, (rows, HD), 1)
    line = lax.broadcasted_iota(jnp.int32, (PAD, HD), 0)
    heads = 2 * share // HD
    codes = jnp.zeros((rows, HD), jnp.float32)
    for h in range(heads):
        one = total[:, h * HD : (h + 1) * HD]
        top = jnp.max(jnp.abs(one), axis=1, keepdims=True)
        code = jnp.ceil(jnp.log2(jnp.maximum(top, 1e-30)) * STEPS) + 1.0
        factor = TOP * jnp.exp2(code * (-1.0 / STEPS))
        scaled = jnp.floor(one * factor + 0.5)
        out_ref[0:rows, h * HD : (h + 1) * HD] = scaled.astype(jnp.int32).astype(jnp.int16)
        codes = jnp.where(lane == h, code, codes)
    kept = [jnp.zeros((PAD, HD), jnp.float32) for _ in range(heads)]
    for g in range(rows // HD):
        turned = codes[g * HD : (g + 1) * HD, :].T
        for h in range(heads):
            kept[h] = jnp.where(line == g, turned[h : h + 1, :], kept[h])
    for h in range(heads):
        out_ref[rows : rows + PAD, h * HD : (h + 1) * HD] = kept[h].astype(jnp.int32).astype(jnp.int16)


def project_body(*refs, jobs, share):
    outs = refs[-len(jobs) :]
    for (f, r, fp, w, wp, far), out_ref in zip(jobs, outs):
        m = refs[fp].shape[1]
        width = refs[fp].shape[2]
        own = refs[f][:, r : r + m, :].reshape(TPD * m, width)
        other = refs[fp][...].reshape(TPD * m, width)
        total = jnp.dot(own, refs[w][...], preferred_element_type=jnp.float32)
        total += jnp.dot(other, refs[wp][...], preferred_element_type=jnp.float32)
        if far:
            encode(total, out_ref, share)
        else:
            out_ref[...] = total


def project(feats, jobs, share):
    inputs, listed, shapes = [feats], [], []

    def at(x):
        for i, y in enumerate(inputs):
            if x is y:
                return i
        inputs.append(x)
        return len(inputs) - 1

    flops = 0
    for (r, m), block, w, wp, far in jobs:
        rows = TPD * m
        listed.append((0, r, at(block), at(w), at(wp), far))
        shape = ((rows + PAD, 2 * share), jnp.int16) if far else ((rows, 2 * share), jnp.float32)
        shapes.append(jax.ShapeDtypeStruct(*shape))
        flops += 8 * rows * feats.shape[2] * share
    return call(
        functools.partial(project_body, jobs=listed, share=share),
        [VMEM] * len(inputs),
        [VMEM] * len(jobs),
        shapes,
        flops,
    )(*inputs)


def finish_body(deal_ref, limit_ref, gain_ref, own_ref, *rest, stage, share, peers, span, mode):
    r0, m = stage
    rows = TPD * m
    groups = lax.axis_size("gx")
    own_index = lax.axis_index("gx")
    codes, outs, scale_ref = rest[:peers], rest[peers:-1], rest[-1]
    heads = 2 * share // HD
    line = lax.broadcasted_iota(jnp.int32, (HD, HD), 0)
    for p in range(peers):
        saved = codes[p][rows : rows + PAD, :].astype(jnp.int32).astype(jnp.float32)
        for g in range(rows // HD):
            stack = jnp.zeros((HD, HD), jnp.float32)
            for h in range(heads):
                stack = jnp.where(line == h, saved[g : g + 1, h * HD : (h + 1) * HD], stack)
            scale_ref[p, g * HD : (g + 1) * HD, :] = jnp.exp2(stack.T * (1.0 / STEPS)) * (1.0 / TOP)
    gain = gain_ref[...]
    position = r0 + lax.broadcasted_iota(jnp.int32, (m, HD), 0)
    first = own_index * TPD
    for k in range(groups):
        taker = k if mode == "a2a" else (own_index + k) % groups
        out = outs[0].at[k] if mode == "a2a" else outs[k]
        for c in range(TPD // span):
            tile = c * span
            for t in range(c * span, (c + 1) * span):
                tile = jnp.where(deal_ref[taker, t] == first + t, t, tile)
            inside = position < limit_ref[first + tile]
            start = pl.multiple_of(tile * m, 16)
            for h in range(heads):
                cols = slice(h * HD, (h + 1) * HD)
                total = own_ref[pl.ds(start, m), cols]
                for p in range(peers):
                    code = codes[p][pl.ds(start, m), cols].astype(jnp.int32).astype(jnp.float32)
                    total += code * scale_ref[p, pl.ds(start, m), h : h + 1]
                if h < heads // 2:
                    mean_square = jnp.mean(total * total, axis=1, keepdims=True)
                    total = total * lax.rsqrt(mean_square + epsilon) * gain
                out[c * m : (c + 1) * m, cols] = jnp.where(inside, total, 0.0).astype(jnp.bfloat16)


def finish(stage, deal, tile_rows, gain, own, codes, groups, share, span, mode):
    rows = TPD * stage[1]
    shape = (TPD // span * stage[1], 2 * share)
    if mode == "a2a":
        shapes = [jax.ShapeDtypeStruct((groups,) + shape, jnp.bfloat16)]
    else:
        shapes = [jax.ShapeDtypeStruct(shape, jnp.bfloat16)] * groups
    body = functools.partial(
        finish_body, stage=stage, share=share, peers=len(codes), span=span, mode=mode
    )
    return call(
        body,
        [SMEM, SMEM, VMEM, VMEM] + [VMEM] * len(codes),
        [VMEM] * len(shapes),
        shapes,
        40 * rows * share,
        [pltpu.VMEM((max(1, len(codes)), rows, HD), jnp.float32)],
    )(deal, tile_rows, gain, own, *codes)


def place_body(deal_ref, *refs, stages, modes, share, span):
    groups = lax.axis_size("gx")
    own_index = lax.axis_index("gx")
    pieces, (keys_ref, values_ref, sem) = list(refs[:-3]), refs[-3:]
    todo = []
    for s, ((r0, m), mode) in enumerate(zip(stages, modes)):
        whole = pieces.pop(0) if mode == "a2a" else None
        for k in range(groups):
            giver = k if mode == "a2a" else (own_index - k + groups) % groups
            piece = whole.at[k] if mode == "a2a" else pieces.pop(0)
            for c in range(TPD // span):
                slot = -1
                for t in range(c * span, (c + 1) * span):
                    slot = jnp.where(deal_ref[own_index, t] // TPD == giver, t, slot)
                row = pl.multiple_of(jnp.maximum(slot, 0) * TILE + r0, 16)
                for i, ref in enumerate((keys_ref, values_ref)):
                    copy = pltpu.make_async_copy(
                        piece.at[c * m : (c + 1) * m, i * share : (i + 1) * share],
                        ref.at[pl.ds(row, m)],
                        sem.at[s, k, c, i],
                    )
                    todo.append((slot, copy))
    for slot, copy in todo:
        pl.when(slot >= 0)(copy.start)
    for slot, copy in todo:
        pl.when(slot >= 0)(copy.wait)


def place(stages, modes, deal, pieces, groups, share, span):
    shape = jax.ShapeDtypeStruct((TPD * TILE, share), jnp.bfloat16)
    return call(
        functools.partial(place_body, stages=stages, modes=modes, share=share, span=span),
        [SMEM] + [VMEM] * len(pieces),
        [ANY, ANY],
        [shape, shape],
        1e6,
        [pltpu.SemaphoreType.DMA((len(stages), groups, TPD // span, 2))],
    )(deal, *pieces)


def local(image_feats, w_kv, k_gain, tile_rows, deal):
    groups = lax.axis_size("gx")
    members = lax.axis_size("gy")
    chips = members // CORES
    share = w_kv.shape[1] // 2 // members
    feats = image_feats.reshape(TPD, TILE, image_feats.shape[1])
    gain = k_gain.reshape(1, HD)
    span = min(TPD, groups)
    stages, modes, row = [], [], 0
    for units, mode in STAGES:
        stages.append((row * 16, units * 16))
        modes.append(mode)
        row += units

    def swap(x):
        return lax.ppermute(x, "gy", [(g, g ^ 1) for g in range(members)])

    def along(x, k):
        pairs = [
            (x0 * CORES + c, (x0 + k) % chips * CORES + c) for x0 in range(chips) for c in range(CORES)
        ]
        return lax.ppermute(x, "gy", pairs)

    n = len(stages)
    f0, w_far, w_send = prepare(feats, w_kv, stages[:1], range(1, chips), share)
    v_far = [swap(w) for w in w_send]
    near = [swap(f) for f in f0]
    f1, (w_near,), w_send = prepare(feats, w_kv, stages[1:], (0,), share)
    near += [swap(f) for f in f1]
    v_near = swap(w_send[0])

    def far_jobs(s):
        return [(stages[s], near[s], w_far[k], v_far[k], True) for k in range(chips - 1)]

    def own_job(s):
        return [(stages[s], near[s], w_near, v_near, False)]

    codes, own = [None] * n, [None] * n
    for s in range(n):
        jobs = far_jobs(s) + (own_job(s - 1) if s else []) + (own_job(s) if s == n - 1 else [])
        got = project(feats, jobs, share)
        codes[s] = [along(x, k + 1) for k, x in enumerate(got[: chips - 1])]
        if s:
            own[s - 1] = got[chips - 1]
            own[s] = got[-1]
    pieces = []
    for s in range(n):
        laid = finish(
            stages[s], deal, tile_rows, gain, own[s], codes[s], groups, share, span, modes[s]
        )
        if modes[s] == "a2a":
            pieces.append(lax.all_to_all(laid[0], "gx", 0, 0, tiled=True))
            continue
        for k, x in enumerate(laid):
            pairs = [(i, (i + k) % groups) for i in range(groups)]
            pieces.append(lax.ppermute(x, "gx", pairs) if k else x)
    return tuple(place(stages, modes, deal, pieces, groups, share, span))


def solution(mesh):
    placed = (P("gx", "gy"), P("gy", None), P(), P(), P())

    return jax.shard_map(local, mesh=mesh, in_specs=placed, out_specs=(P("gx", "gy"), P("gx", "gy")), check_vma=False)
```

```python
import functools

import jax
import jax.numpy as jnp
from jax import lax
from jax.experimental import pallas as pl
from jax.experimental.pallas import tpu as pltpu
from jax.sharding import PartitionSpec as P


HD = 128
TILE = 128
TPD = 16
CORES = 2
epsilon = 1e-05

STEPS = 64.0
TOP = 32700.0
PAD = 16

VMEM = pl.BlockSpec(memory_space=pltpu.VMEM)
SMEM = pl.BlockSpec(memory_space=pltpu.SMEM)
ANY = pl.BlockSpec(memory_space=pl.ANY)
HBM = pl.BlockSpec(memory_space=pltpu.HBM)


def call(body, ins, outs, shapes, flops, scratch=(), aliases={}):
    nbytes = sum(s.size * s.dtype.itemsize for s in shapes)
    return pl.pallas_call(
        body,
        in_specs=ins,
        out_specs=outs,
        out_shape=shapes,
        scratch_shapes=scratch,
        input_output_aliases=aliases,
        compiler_params=pltpu.CompilerParams(vmem_limit_bytes=16 * 2**20),
        cost_estimate=pl.CostEstimate(flops=int(flops), bytes_accessed=2 * nbytes, transcendentals=0),
    )


STAGES = ((2, "permute"), (2, "a2a"), (2, "permute"), (2, "a2a"))


def target(k):
    chips = lax.axis_size("gy") // CORES
    member = lax.axis_index("gy")
    chip, core = member // CORES, member % CORES
    there = (chip + k) % chips * CORES
    return there + core, there + 1 - core


def run_all(copies):
    for c in copies:
        c.start()
    for c in copies:
        c.wait()


def prepare_body(f_ref, w_ref, *refs, stages, ks, share):
    feats, weights, sem = refs[: len(stages)], refs[len(stages) : -1], refs[-1]
    members = lax.axis_size("gy")
    copies = []
    for i, k in enumerate(ks):
        for j, which in enumerate(target(k)):
            if k and j:
                continue
            w_out = weights[i] if not j else weights[len(ks)]
            for part in range(2):
                start = pl.multiple_of((part * members + which) * share, share)
                copies.append((w_ref.at[:, pl.ds(start, share)], w_out.at[:, part * share : (part + 1) * share]))
    for (r, m), f_out in zip(stages, feats):
        copies.append((f_ref.at[:, r : r + m], f_out))
    run_all([pltpu.make_async_copy(a, b, sem.at[i]) for i, (a, b) in enumerate(copies)])


def prepare(feats, w_kv, stages, ks, share):
    width = feats.shape[2]
    shapes = [jax.ShapeDtypeStruct((TPD, m, width), feats.dtype) for _, m in stages]
    shapes += [jax.ShapeDtypeStruct((width, 2 * share), w_kv.dtype) for _ in range(len(ks) + 1)]
    body = functools.partial(prepare_body, stages=stages, ks=ks, share=share)
    sems = [pltpu.SemaphoreType.DMA((len(stages) + 4 * len(ks),))]
    got = call(body, [HBM, HBM], [VMEM] * len(shapes), shapes, 1e6, sems)(feats, w_kv)
    weights = got[len(stages) :]
    return got[: len(stages)], weights[: len(ks)], weights[len(ks) :]


def encode(total, out_ref, share):
    rows = total.shape[0]
    lane = lax.broadcasted_iota(jnp.int32, (rows, HD), 1)
    line = lax.broadcasted_iota(jnp.int32, (PAD, HD), 0)
    heads = 2 * share // HD
    codes = jnp.zeros((rows, HD), jnp.float32)
    for h in range(heads):
        one = total[:, h * HD : (h + 1) * HD]
        top = jnp.max(jnp.abs(one), axis=1, keepdims=True)
        code = jnp.ceil(jnp.log2(jnp.maximum(top, 1e-30)) * STEPS) + 1.0
        factor = TOP * jnp.exp2(code * (-1.0 / STEPS))
        scaled = jnp.floor(one * factor + 0.5)
        out_ref[0:rows, h * HD : (h + 1) * HD] = scaled.astype(jnp.int32).astype(jnp.int16)
        codes = jnp.where(lane == h, code, codes)
    kept = [jnp.zeros((PAD, HD), jnp.float32) for _ in range(heads)]
    for g in range(rows // HD):
        turned = codes[g * HD : (g + 1) * HD, :].T
        for h in range(heads):
            kept[h] = jnp.where(line == g, turned[h : h + 1, :], kept[h])
    for h in range(heads):
        out_ref[rows : rows + PAD, h * HD : (h + 1) * HD] = kept[h].astype(jnp.int32).astype(jnp.int16)


def project_body(*refs, jobs, share):
    outs = refs[-len(jobs) :]
    for (f, r, fp, w, wp, far), out_ref in zip(jobs, outs):
        m = refs[fp].shape[1]
        width = refs[fp].shape[2]
        own = refs[f][:, r : r + m, :].reshape(TPD * m, width)
        other = refs[fp][...].reshape(TPD * m, width)
        total = jnp.dot(own, refs[w][...], preferred_element_type=jnp.float32)
        total += jnp.dot(other, refs[wp][...], preferred_element_type=jnp.float32)
        if far:
            encode(total, out_ref, share)
        else:
            out_ref[...] = total


def project(feats, jobs, share):
    inputs, listed, shapes = [feats], [], []

    def at(x):
        for i, y in enumerate(inputs):
            if x is y:
                return i
        inputs.append(x)
        return len(inputs) - 1

    flops = 0
    for (r, m), block, w, wp, far in jobs:
        rows = TPD * m
        listed.append((0, r, at(block), at(w), at(wp), far))
        shape = ((rows + PAD, 2 * share), jnp.int16) if far else ((rows, 2 * share), jnp.float32)
        shapes.append(jax.ShapeDtypeStruct(*shape))
        flops += 8 * rows * feats.shape[2] * share
    return call(
        functools.partial(project_body, jobs=listed, share=share),
        [VMEM] * len(inputs),
        [VMEM] * len(jobs),
        shapes,
        flops,
    )(*inputs)


def split(x, parts):
    terms = []
    for _ in range(parts):
        term = x.astype(jnp.bfloat16)
        terms.append(term)
        x = x - term.astype(jnp.float32)
    return jnp.concatenate(terms, axis=1)


def finish_body(deal_ref, limit_ref, gain_ref, own_ref, *rest, stage, share, peers, span, mode):
    r0, m = stage
    rows = TPD * m
    groups = lax.axis_size("gx")
    own_index = lax.axis_index("gx")
    codes, outs, (saved_ref, done_ref) = rest[:peers], rest[peers:-2], rest[-2:]
    heads = 2 * share // HD
    for p in range(peers):
        saved_ref[p] = codes[p][rows : rows + PAD, :].astype(jnp.int32).astype(jnp.float32)
    line = lax.broadcasted_iota(jnp.int32, (HD, HD), 0)
    at_head = lax.broadcasted_iota(jnp.int32, (3 * HD, 2 * share), 0) % HD
    to_head = lax.broadcasted_iota(jnp.int32, (3 * HD, 2 * share), 1) // HD
    spread = jnp.where(at_head == to_head, 1.0, 0.0).astype(jnp.bfloat16)
    ones = jnp.ones((2 * HD, HD), jnp.bfloat16)
    gain = gain_ref[...]

    def block(g, carry):
        at = pl.ds(pl.multiple_of(g * HD, HD), HD)
        total = own_ref[at, :]
        for p in range(peers):
            saved = saved_ref[p, pl.ds(g, 1), :]
            stack = jnp.zeros((HD, HD), jnp.float32)
            for h in range(heads):
                stack = jnp.where(line == h, saved[:, h * HD : (h + 1) * HD], stack)
            scale = jnp.exp2(stack.T * (1.0 / STEPS)) * (1.0 / TOP)
            wide = jnp.dot(split(scale, 3), spread, preferred_element_type=jnp.float32)
            total += codes[p][at, :].astype(jnp.int32).astype(jnp.float32) * wide
        for h in range(heads):
            cols = slice(h * HD, (h + 1) * HD)
            part = total[:, cols]
            if h < heads // 2:
                squares = jnp.dot(split(part * part, 2), ones, preferred_element_type=jnp.float32)
                part = part * lax.rsqrt(squares * (1.0 / HD) + epsilon) * gain
            done_ref[at, cols] = part
        return carry

    lax.fori_loop(0, rows // HD, block, 0, unroll=2)
    position = r0 + lax.broadcasted_iota(jnp.int32, (m, 2 * share), 0)
    first = own_index * TPD
    for k in range(groups):
        taker = k if mode == "a2a" else (own_index + k) % groups
        out = outs[0].at[k] if mode == "a2a" else outs[k]
        for c in range(TPD // span):
            tile = c * span
            for t in range(c * span, (c + 1) * span):
                tile = jnp.where(deal_ref[taker, t] == first + t, t, tile)
            kept = done_ref[pl.ds(pl.multiple_of(tile * m, 16), m), :]
            kept = jnp.where(position < limit_ref[first + tile], kept, 0.0)
            out[c * m : (c + 1) * m, :] = kept.astype(jnp.bfloat16)


def finish(stage, deal, tile_rows, gain, own, codes, groups, share, span, mode):
    rows = TPD * stage[1]
    shape = (TPD // span * stage[1], 2 * share)
    if mode == "a2a":
        shapes = [jax.ShapeDtypeStruct((groups,) + shape, jnp.bfloat16)]
    else:
        shapes = [jax.ShapeDtypeStruct(shape, jnp.bfloat16)] * groups
    body = functools.partial(
        finish_body, stage=stage, share=share, peers=len(codes), span=span, mode=mode
    )
    return call(
        body,
        [SMEM, SMEM, VMEM, VMEM] + [VMEM] * len(codes),
        [VMEM] * len(shapes),
        shapes,
        40 * rows * share,
        [
            pltpu.VMEM((max(1, len(codes)), PAD, 2 * share), jnp.float32),
            pltpu.VMEM((rows, 2 * share), jnp.float32),
        ],
    )(deal, tile_rows, gain, own, *codes)


def place_body(deal_ref, *refs, stages, modes, share, span, held):
    groups = lax.axis_size("gx")
    own_index = lax.axis_index("gx")
    pieces, (keys_ref, values_ref, sem) = list(refs[:-3]), refs[-3:]
    if held:
        pieces = pieces[:-2]
    todo = []
    for s, ((r0, m), mode) in enumerate(zip(stages, modes)):
        whole = pieces.pop(0) if mode == "a2a" else None
        for k in range(groups):
            giver = k if mode == "a2a" else (own_index - k + groups) % groups
            piece = whole.at[k] if mode == "a2a" else pieces.pop(0)
            for c in range(TPD // span):
                slot = -1
                for t in range(c * span, (c + 1) * span):
                    slot = jnp.where(deal_ref[own_index, t] // TPD == giver, t, slot)
                row = pl.multiple_of(jnp.maximum(slot, 0) * TILE + r0, 16)
                for i, ref in enumerate((keys_ref, values_ref)):
                    copy = pltpu.make_async_copy(
                        piece.at[c * m : (c + 1) * m, i * share : (i + 1) * share],
                        ref.at[pl.ds(row, m)],
                        sem.at[s, k, c, i],
                    )
                    todo.append((slot, copy))
    for slot, copy in todo:
        pl.when(slot >= 0)(copy.start)
    for slot, copy in todo:
        pl.when(slot >= 0)(copy.wait)


def place(stages, modes, deal, pieces, groups, share, span, before=()):
    shape = jax.ShapeDtypeStruct((TPD * TILE, share), jnp.bfloat16)
    n = len(pieces)
    return call(
        functools.partial(
            place_body, stages=stages, modes=modes, share=share, span=span, held=bool(before)
        ),
        [SMEM] + [VMEM] * n + [ANY] * len(before),
        [ANY, ANY],
        [shape, shape],
        1e6,
        [pltpu.SemaphoreType.DMA((len(stages), groups, TPD // span, 2))],
        {n + 1: 0, n + 2: 1} if before else {},
    )(deal, *pieces, *before)


def local(image_feats, w_kv, k_gain, tile_rows, deal):
    groups = lax.axis_size("gx")
    members = lax.axis_size("gy")
    chips = members // CORES
    share = w_kv.shape[1] // 2 // members
    feats = image_feats.reshape(TPD, TILE, image_feats.shape[1])
    gain = k_gain.reshape(1, HD)
    span = min(TPD, groups)
    stages, modes, row = [], [], 0
    for units, mode in STAGES:
        stages.append((row * 16, units * 16))
        modes.append(mode)
        row += units

    def swap(x):
        return lax.ppermute(x, "gy", [(g, g ^ 1) for g in range(members)])

    def along(x, k):
        pairs = [
            (x0 * CORES + c, (x0 + k) % chips * CORES + c) for x0 in range(chips) for c in range(CORES)
        ]
        return lax.ppermute(x, "gy", pairs)

    n = len(stages)

    def cut(which):
        starts = (which * share, (members + which) * share)
        parts = [lax.dynamic_slice(w_kv, (0, start), (w_kv.shape[0], share)) for start in starts]
        return jnp.concatenate(parts, axis=1)

    f0 = feats[:, stages[0][0] : sum(stages[0])]
    w_send = [cut(target(k)[1]) for k in range(1, chips)]
    near = [swap(f0)]
    v_far = [swap(w) for w in w_send]
    f1, w_own, w_send = prepare(feats, w_kv, stages[1:], range(chips), share)
    w_near, w_far = w_own[0], w_own[1:]
    near += [swap(f) for f in f1]
    v_near = swap(w_send[0])

    def far_jobs(s):
        return [(stages[s], near[s], w_far[k], v_far[k], True) for k in range(chips - 1)]

    def own_job(s):
        return [(stages[s], near[s], w_near, v_near, False)]

    codes, own = [None] * n, [None] * n
    for s in range(n):
        jobs = far_jobs(s) + (own_job(s - 1) if s else []) + (own_job(s) if s == n - 1 else [])
        got = project(feats, jobs, share)
        codes[s] = [along(x, k + 1) for k, x in enumerate(got[: chips - 1])]
        if s:
            own[s - 1] = got[chips - 1]
            own[s] = got[-1]
    pieces = [[] for _ in range(n)]
    for s in range(n):
        laid = finish(
            stages[s], deal, tile_rows, gain, own[s], codes[s], groups, share, span, modes[s]
        )
        if modes[s] == "a2a":
            pieces[s].append(lax.all_to_all(laid[0], "gx", 0, 0, tiled=True))
            continue
        for k, x in enumerate(laid):
            pairs = [(i, (i + k) % groups) for i in range(groups)]
            pieces[s].append(lax.ppermute(x, "gx", pairs) if k else x)
    early = n - 1
    out = place(stages[:early], modes[:early], deal, sum(pieces[:early], []), groups, share, span)
    return tuple(place(stages[early:], modes[early:], deal, sum(pieces[early:], []), groups, share, span, out))


def solution(mesh):
    placed = (P("gx", "gy"), P("gy", None), P(), P(), P())

    return jax.shard_map(local, mesh=mesh, in_specs=placed, out_specs=(P("gx", "gy"), P("gx", "gy")), check_vma=False)
```

```python
import functools

import jax
import jax.numpy as jnp
from jax import lax
from jax.experimental import pallas as pl
from jax.experimental.pallas import tpu as pltpu
from jax.sharding import PartitionSpec as P


HD = 128
TILE = 128
TPD = 16
CORES = 2
epsilon = 1e-05

STEPS = 64.0
TOP = 32700.0
PAD = 16

VMEM = pl.BlockSpec(memory_space=pltpu.VMEM)
SMEM = pl.BlockSpec(memory_space=pltpu.SMEM)
ANY = pl.BlockSpec(memory_space=pl.ANY)
HBM = pl.BlockSpec(memory_space=pltpu.HBM)


def call(body, ins, outs, shapes, flops, scratch=(), aliases={}):
    nbytes = sum(s.size * s.dtype.itemsize for s in shapes)
    return pl.pallas_call(
        body,
        in_specs=ins,
        out_specs=outs,
        out_shape=shapes,
        scratch_shapes=scratch,
        input_output_aliases=aliases,
        compiler_params=pltpu.CompilerParams(vmem_limit_bytes=8 * 2**20),
        cost_estimate=pl.CostEstimate(flops=int(flops), bytes_accessed=2 * nbytes, transcendentals=0),
    )


STAGES = ((2, "permute"), (2, "a2a"), (2, "permute"), (2, "a2a"))


def target(k):
    chips = lax.axis_size("gy") // CORES
    member = lax.axis_index("gy")
    chip, core = member // CORES, member % CORES
    there = (chip + k) % chips * CORES
    return there + core, there + 1 - core


def run_all(copies):
    for c in copies:
        c.start()
    for c in copies:
        c.wait()


def prepare_body(f_ref, w_ref, *refs, stages, ks, share):
    feats, weights, sem = refs[: len(stages)], refs[len(stages) : -1], refs[-1]
    members = lax.axis_size("gy")
    copies = []
    for i, k in enumerate(ks):
        for j, which in enumerate(target(k)):
            if k and j:
                continue
            w_out = weights[i] if not j else weights[len(ks)]
            for part in range(2):
                start = pl.multiple_of((part * members + which) * share, share)
                copies.append((w_ref.at[:, pl.ds(start, share)], w_out.at[:, part * share : (part + 1) * share]))
    for (r, m), f_out in zip(stages, feats):
        copies.append((f_ref.at[:, r : r + m], f_out))
    run_all([pltpu.make_async_copy(a, b, sem.at[i]) for i, (a, b) in enumerate(copies)])


def prepare(feats, w_kv, stages, ks, share):
    width = feats.shape[2]
    shapes = [jax.ShapeDtypeStruct((TPD, m, width), feats.dtype) for _, m in stages]
    shapes += [jax.ShapeDtypeStruct((width, 2 * share), w_kv.dtype) for _ in range(len(ks) + 1)]
    body = functools.partial(prepare_body, stages=stages, ks=ks, share=share)
    sems = [pltpu.SemaphoreType.DMA((len(stages) + 4 * len(ks),))]
    got = call(body, [HBM, HBM], [VMEM] * len(shapes), shapes, 1e6, sems)(feats, w_kv)
    weights = got[len(stages) :]
    return got[: len(stages)], weights[: len(ks)], weights[len(ks) :]


def encode(total, out_ref, share):
    rows = total.shape[0]
    lane = lax.broadcasted_iota(jnp.int32, (rows, HD), 1)
    line = lax.broadcasted_iota(jnp.int32, (PAD, HD), 0)
    heads = 2 * share // HD
    codes = jnp.zeros((rows, HD), jnp.float32)
    for h in range(heads):
        one = total[:, h * HD : (h + 1) * HD]
        top = jnp.max(jnp.abs(one), axis=1, keepdims=True)
        code = jnp.ceil(jnp.log2(jnp.maximum(top, 1e-30)) * STEPS) + 1.0
        factor = TOP * jnp.exp2(code * (-1.0 / STEPS))
        scaled = jnp.floor(one * factor + 0.5)
        out_ref[0:rows, h * HD : (h + 1) * HD] = scaled.astype(jnp.int32).astype(jnp.int16)
        codes = jnp.where(lane == h, code, codes)
    kept = [jnp.zeros((PAD, HD), jnp.float32) for _ in range(heads)]
    for g in range(rows // HD):
        turned = codes[g * HD : (g + 1) * HD, :].T
        for h in range(heads):
            kept[h] = jnp.where(line == g, turned[h : h + 1, :], kept[h])
    for h in range(heads):
        out_ref[rows : rows + PAD, h * HD : (h + 1) * HD] = kept[h].astype(jnp.int32).astype(jnp.int16)


def project_body(*refs, jobs, share):
    outs = refs[-len(jobs) :]
    for (f, r, fp, w, wp, far), out_ref in zip(jobs, outs):
        m = refs[fp].shape[1]
        width = refs[fp].shape[2]
        own = refs[f][:, r : r + m, :].reshape(TPD * m, width)
        other = refs[fp][...].reshape(TPD * m, width)
        total = jnp.dot(own, refs[w][...], preferred_element_type=jnp.float32)
        total += jnp.dot(other, refs[wp][...], preferred_element_type=jnp.float32)
        if far:
            encode(total, out_ref, share)
        else:
            out_ref[...] = total


def project(feats, jobs, share):
    inputs, listed, shapes = [feats], [], []

    def at(x):
        for i, y in enumerate(inputs):
            if x is y:
                return i
        inputs.append(x)
        return len(inputs) - 1

    flops = 0
    for (r, m), block, w, wp, far in jobs:
        rows = TPD * m
        listed.append((0, r, at(block), at(w), at(wp), far))
        shape = ((rows + PAD, 2 * share), jnp.int16) if far else ((rows, 2 * share), jnp.float32)
        shapes.append(jax.ShapeDtypeStruct(*shape))
        flops += 8 * rows * feats.shape[2] * share
    return call(
        functools.partial(project_body, jobs=listed, share=share),
        [VMEM] * len(inputs),
        [VMEM] * len(jobs),
        shapes,
        flops,
    )(*inputs)


def split(x, parts):
    terms = []
    for _ in range(parts):
        term = x.astype(jnp.bfloat16)
        terms.append(term)
        x = x - term.astype(jnp.float32)
    return jnp.concatenate(terms, axis=1)


def finish_body(deal_ref, limit_ref, gain_ref, own_ref, *rest, stage, share, peers, span, mode):
    r0, m = stage
    rows = TPD * m
    groups = lax.axis_size("gx")
    own_index = lax.axis_index("gx")
    codes, outs, (saved_ref, done_ref) = rest[:peers], rest[peers:-2], rest[-2:]
    heads = 2 * share // HD
    for p in range(peers):
        saved_ref[p] = codes[p][rows : rows + PAD, :].astype(jnp.int32).astype(jnp.float32)
    line = lax.broadcasted_iota(jnp.int32, (HD, HD), 0)
    at_head = lax.broadcasted_iota(jnp.int32, (3 * HD, 2 * share), 0) % HD
    to_head = lax.broadcasted_iota(jnp.int32, (3 * HD, 2 * share), 1) // HD
    spread = jnp.where(at_head == to_head, 1.0, 0.0).astype(jnp.bfloat16)
    ones = jnp.ones((2 * HD, HD), jnp.bfloat16)
    gain = gain_ref[...]

    def block(g, carry):
        at = pl.ds(pl.multiple_of(g * HD, HD), HD)
        total = own_ref[at, :]
        for p in range(peers):
            saved = saved_ref[p, pl.ds(g, 1), :]
            stack = jnp.zeros((HD, HD), jnp.float32)
            for h in range(heads):
                stack = jnp.where(line == h, saved[:, h * HD : (h + 1) * HD], stack)
            scale = jnp.exp2(stack.T * (1.0 / STEPS)) * (1.0 / TOP)
            wide = jnp.dot(split(scale, 3), spread, preferred_element_type=jnp.float32)
            total += codes[p][at, :].astype(jnp.int32).astype(jnp.float32) * wide
        for h in range(heads):
            cols = slice(h * HD, (h + 1) * HD)
            part = total[:, cols]
            if h < heads // 2:
                squares = jnp.dot(split(part * part, 2), ones, preferred_element_type=jnp.float32)
                part = part * lax.rsqrt(squares * (1.0 / HD) + epsilon) * gain
            done_ref[at, cols] = part
        return carry

    lax.fori_loop(0, rows // HD, block, 0, unroll=4)
    position = r0 + lax.broadcasted_iota(jnp.int32, (m, 2 * share), 0)
    first = own_index * TPD
    for k in range(groups):
        taker = k if mode == "a2a" else (own_index + k) % groups
        out = outs[0].at[k] if mode == "a2a" else outs[k]
        for c in range(TPD // span):
            tile = c * span
            for t in range(c * span + 1, (c + 1) * span):
                tile += jnp.where(deal_ref[taker, t] == first + t, t - c * span, 0)
            kept = done_ref[pl.ds(pl.multiple_of(tile * m, 16), m), :]
            kept = jnp.where(position < limit_ref[first + tile], kept, 0.0)
            out[c * m : (c + 1) * m, :] = kept.astype(jnp.bfloat16)


def finish(stage, deal, tile_rows, gain, own, codes, groups, share, span, mode):
    rows = TPD * stage[1]
    shape = (TPD // span * stage[1], 2 * share)
    if mode == "a2a":
        shapes = [jax.ShapeDtypeStruct((groups,) + shape, jnp.bfloat16)]
    else:
        shapes = [jax.ShapeDtypeStruct(shape, jnp.bfloat16)] * groups
    body = functools.partial(
        finish_body, stage=stage, share=share, peers=len(codes), span=span, mode=mode
    )
    return call(
        body,
        [SMEM, SMEM, VMEM, VMEM] + [VMEM] * len(codes),
        [VMEM] * len(shapes),
        shapes,
        40 * rows * share,
        [
            pltpu.VMEM((max(1, len(codes)), PAD, 2 * share), jnp.float32),
            pltpu.VMEM((rows, 2 * share), jnp.float32),
        ],
    )(deal, tile_rows, gain, own, *codes)


def place_body(deal_ref, *refs, stages, modes, share, span, held):
    groups = lax.axis_size("gx")
    own_index = lax.axis_index("gx")
    pieces, (keys_ref, values_ref, sem) = list(refs[:-3]), refs[-3:]
    if held:
        pieces = pieces[:-2]
    todo = []
    for s, ((r0, m), mode) in enumerate(zip(stages, modes)):
        whole = pieces.pop(0) if mode == "a2a" else None
        for k in range(groups):
            giver = k if mode == "a2a" else (own_index - k + groups) % groups
            piece = whole.at[k] if mode == "a2a" else pieces.pop(0)
            for c in range(TPD // span):
                slot = -1
                for t in range(c * span, (c + 1) * span):
                    slot = jnp.where(deal_ref[own_index, t] // TPD == giver, t, slot)
                row = pl.multiple_of(jnp.maximum(slot, 0) * TILE + r0, 16)
                for i, ref in enumerate((keys_ref, values_ref)):
                    copy = pltpu.make_async_copy(
                        piece.at[c * m : (c + 1) * m, i * share : (i + 1) * share],
                        ref.at[pl.ds(row, m)],
                        sem.at[s, k, c, i],
                    )
                    todo.append((slot, copy))
    for slot, copy in todo:
        pl.when(slot >= 0)(copy.start)
    for slot, copy in todo:
        pl.when(slot >= 0)(copy.wait)


def place(stages, modes, deal, pieces, groups, share, span, before=()):
    shape = jax.ShapeDtypeStruct((TPD * TILE, share), jnp.bfloat16)
    n = len(pieces)
    return call(
        functools.partial(
            place_body, stages=stages, modes=modes, share=share, span=span, held=bool(before)
        ),
        [SMEM] + [VMEM] * n + [ANY] * len(before),
        [ANY, ANY],
        [shape, shape],
        1e6,
        [pltpu.SemaphoreType.DMA((len(stages), groups, TPD // span, 2))],
        {n + 1: 0, n + 2: 1} if before else {},
    )(deal, *pieces, *before)


def local(image_feats, w_kv, k_gain, tile_rows, deal):
    groups = lax.axis_size("gx")
    members = lax.axis_size("gy")
    chips = members // CORES
    share = w_kv.shape[1] // 2 // members
    feats = image_feats.reshape(TPD, TILE, image_feats.shape[1])
    gain = k_gain.reshape(1, HD)
    span = min(TPD, groups)
    stages, modes, row = [], [], 0
    for units, mode in STAGES:
        stages.append((row * 16, units * 16))
        modes.append(mode)
        row += units

    def swap(x):
        return lax.ppermute(x, "gy", [(g, g ^ 1) for g in range(members)])

    def along(x, k):
        pairs = [
            (x0 * CORES + c, (x0 + k) % chips * CORES + c) for x0 in range(chips) for c in range(CORES)
        ]
        return lax.ppermute(x, "gy", pairs)

    n = len(stages)

    def cut(which):
        starts = (which * share, (members + which) * share)
        parts = [lax.dynamic_slice(w_kv, (0, start), (w_kv.shape[0], share)) for start in starts]
        return jnp.concatenate(parts, axis=1)

    f0 = feats[:, stages[0][0] : sum(stages[0])]
    w_send = [cut(target(k)[1]) for k in range(1, chips)]
    near = [swap(f0)]
    v_far = [swap(w) for w in w_send]
    f1, w_own, w_send = prepare(feats, w_kv, stages[1:], range(chips), share)
    w_near, w_far = w_own[0], w_own[1:]
    near += [swap(f) for f in f1]
    v_near = swap(w_send[0])

    def far_jobs(s):
        return [(stages[s], near[s], w_far[k], v_far[k], True) for k in range(chips - 1)]

    def own_job(s):
        return [(stages[s], near[s], w_near, v_near, False)]

    codes, own = [None] * n, [None] * n
    for s in range(n):
        jobs = far_jobs(s) + (own_job(s - 1) if s else []) + (own_job(s) if s == n - 1 else [])
        got = project(feats, jobs, share)
        codes[s] = [along(x, k + 1) for k, x in enumerate(got[: chips - 1])]
        if s:
            own[s - 1] = got[chips - 1]
            own[s] = got[-1]
    pieces = [[] for _ in range(n)]
    for s in range(n):
        laid = finish(
            stages[s], deal, tile_rows, gain, own[s], codes[s], groups, share, span, modes[s]
        )
        if modes[s] == "a2a":
            pieces[s].append(lax.all_to_all(laid[0], "gx", 0, 0, tiled=True))
            continue
        for k, x in enumerate(laid):
            pairs = [(i, (i + k) % groups) for i in range(groups)]
            pieces[s].append(lax.ppermute(x, "gx", pairs) if k else x)
    early = n - 1
    out = place(stages[:early], modes[:early], deal, sum(pieces[:early], []), groups, share, span)
    return tuple(place(stages[early:], modes[early:], deal, sum(pieces[early:], []), groups, share, span, out))


def solution(mesh):
    placed = (P("gx", "gy"), P("gy", None), P(), P(), P())

    return jax.shard_map(local, mesh=mesh, in_specs=placed, out_specs=(P("gx", "gy"), P("gx", "gy")), check_vma=False)
```
